1024 devices in a mesh: node: 32 (over z_hi, y), dev: 32 (over x, z_lo, core).
Axes of the slice: x: 8, y: 8, z: 8 (z_hi: 4, z_lo: 2; z = z_hi * 2 + z_lo), core: 2. Of those that a mesh axis runs over, the one named last changes fastest.
Arguments:
- tokens: bfloat16 [4096, 5120], P(('node', 'dev')), may hold values from -6 to 6
- node_pick: int32 [4096, 3], P(('node', 'dev')), may hold values from 0 to 31, as said below
- expert_pick: int32 [4096, 6], P(('node', 'dev')), may hold values from 0 to 3, as said below
- gate_weight: bfloat16 [4096, 6], P(('node', 'dev')), may hold values from 0.099609375 to 1
- w_gate: bfloat16 [98304, 5120], P(('node', 'dev')), may hold values from -0.078125 to 0.078125
- w_up: bfloat16 [98304, 5120], P(('node', 'dev')), may hold values from -0.078125 to 0.078125
- w_down: bfloat16 [98304, 5120], P(('node', 'dev')), may hold values from -0.21875 to 0.21875
Outputs:
- mixed_out: bfloat16 [4096, 5120], P(('node', 'dev'))
The draws below stay inside these ranges and needn't reach their ends.
Inputs may be any that keep to these rules, and one draw needn't show every extreme that they name: `node_pick`: A token's three nodes differ. On every device at most 2 of its 4 tokens choose one node, and some node is chosen by exactly 2 of them. `expert_pick`: columns 2k and 2k + 1 name two different experts of node node_pick[t, k]. Among the tokens of all devices with one index along dev, at most 12 of those choosing one node pick one same expert of it; this is reached somewhere in every draw.
All inputs are finite; a program needn't handle non-finite values.
Results may differ from the reference program's by a relative error of at most 0.009.
Values may be sent and summed in bfloat16 or wider, within the bound.
No kernel may reach another device: no remote copies, remote signals or barrier semaphores. Data moves between devices by JAX's collectives and lax.ppermute only.
A program may use at most 64 MiB of HBM per device.

```python
import math
import jax
import jax.numpy as jnp
from jax import lax

D = 5120
FF = 768
EXP_NODE = 4
TOK_DEV = 4
CYCLE = 6
CB = 12
EXPERTS = 128
TOKENS = 4096
N_NODE = 32
N_DEV = 32


def routing(key):
    slot_count = 3 * TOK_DEV
    offset_keys = jax.random.split(jax.random.fold_in(key, 101), N_DEV)
    offsets = jax.vmap(lambda sub_key: jax.random.permutation(sub_key, N_NODE)[:CYCLE])(offset_keys)
    source = jnp.arange(N_NODE, dtype=jnp.int32)[:, None, None]
    slot_ids = jnp.arange(slot_count, dtype=jnp.int32) % CYCLE
    chosen = (source + offsets[None, :, slot_ids].astype(jnp.int32)) % N_NODE
    hot_local = jax.random.randint(jax.random.fold_in(key, 102), (N_NODE * N_DEV,), 0, EXP_NODE)
    hot_flag = jax.random.randint(jax.random.fold_in(key, 103), (N_NODE * N_DEV,), 0, 2)
    hot_flag = jnp.maximum(hot_flag, (jnp.arange(N_NODE * N_DEV) == 0).astype(jnp.int32))
    column = jnp.arange(N_DEV, dtype=jnp.int32)[None, :, None]
    receiver = chosen * N_DEV + column
    hot_here = hot_local[receiver]
    flag_here = hot_flag[receiver]
    shape = (N_NODE, N_DEV, slot_count)
    free_pick = jax.random.randint(jax.random.fold_in(key, 104), shape, 0, EXP_NODE)
    step_pick = jax.random.randint(jax.random.fold_in(key, 105), shape, 0, EXP_NODE - 1)
    first_pick = jnp.where(flag_here == 1, hot_here, free_pick)
    second = (first_pick + 1 + step_pick) % EXP_NODE
    node_ids = chosen.reshape(TOKENS, 3).astype(jnp.int32)
    local_ids = jnp.stack([first_pick, second], axis=-1).reshape(TOKENS, 6).astype(jnp.int32)
    return (node_ids, local_ids)


def draw_node_pick(key, part):
    return routing(key)[0]


def draw_expert_pick(key, part):
    return routing(key)[1]


def block_scale(own_key, extent, cuts, smallest, high):
    level, own = 1.0, jax.random.fold_in(own_key, 6)
    for axis_at, shards_of in cuts:
        heights = jnp.exp(jax.random.uniform(jax.random.fold_in(own, axis_at), (shards_of,), jnp.float32, smallest / len(cuts), high / len(cuts)))
        level = level * jnp.repeat(heights, extent[axis_at] // shards_of).reshape([-1 if axis == axis_at else 1 for axis in range(len(extent))])
    return level


def noise(stream_key, shape, width, reach, pieces=(), kind=jnp.bfloat16):
    gain = block_scale(stream_key, shape, pieces, -0.22, 0.18) if pieces else 1.0
    array = jax.random.normal(stream_key, shape, jnp.float32) * width * gain
    return jnp.minimum(jnp.maximum(array, -reach), reach).astype(kind)


def setup_inputs(seed: int = 0) -> dict:
    arg_keys = jax.random.split(jax.random.key(seed), 8)
    tokens = noise(arg_keys[0], (TOKENS, D), 1.0, 6.0, ((0, 1024),))
    node_pick = draw_node_pick(jax.random.fold_in(arg_keys[7], 71), 0)
    expert_pick = draw_expert_pick(jax.random.fold_in(arg_keys[7], 71), 0)
    gate_weight = jnp.clip(jnp.exp(math.log(1.0) - 2.306499 * jax.random.uniform(arg_keys[3], (TOKENS, 6), jnp.float32) ** block_scale(arg_keys[3], (TOKENS, 6), ((0, 1024),), -0.2, 0.2)), 0.099609375, 1.0).astype(jnp.bfloat16)
    w_gate = noise(arg_keys[4], (EXPERTS * FF, D), D ** -0.5, 0.078125, ((0, 1024),))
    w_up = noise(arg_keys[5], (EXPERTS * FF, D), D ** -0.5, 0.078125, ((0, 1024),))
    w_down = noise(arg_keys[6], (EXPERTS * FF, D), FF ** -0.5, 0.21875, ((0, 1024),))
    return {"tokens": tokens, "node_pick": node_pick, "expert_pick": expert_pick, "gate_weight": gate_weight, "w_gate": w_gate, "w_up": w_up, "w_down": w_down}


def reference(tokens, node_pick, expert_pick, gate_weight, w_gate, w_up, w_down):
    owner_node = jnp.take(node_pick, jnp.arange(6, dtype=jnp.int32) // 2, axis=1)
    expert_ids = (owner_node * EXP_NODE + expert_pick).reshape(-1)
    capacity = N_DEV * CB
    slices = N_DEV // EXP_NODE
    ff_dev = FF // slices

    def per_expert(expert_index, running):
        is_hit = expert_ids == expert_index
        found_idx = jnp.nonzero(is_hit, size=capacity, fill_value=0)[0].astype(jnp.int32)
        is_valid = jnp.arange(capacity) < jnp.sum(is_hit.astype(jnp.int32))
        token_rows = jnp.take(tokens, found_idx // 6, axis=0)
        row_start = (expert_index * FF).astype(jnp.int32)
        gate_rows = lax.dynamic_slice_in_dim(w_gate, row_start, FF, 0)
        up_rows = lax.dynamic_slice_in_dim(w_up, row_start, FF, 0)
        down_rows = lax.dynamic_slice_in_dim(w_down, row_start, FF, 0)
        dims = (((1,), (1,)), ((), ()))
        gate_act = lax.dot_general(token_rows, gate_rows, dims, preferred_element_type=jnp.float32)
        up_act = lax.dot_general(token_rows, up_rows, dims, preferred_element_type=jnp.float32)
        hidden = (jax.nn.silu(gate_act) * up_act).astype(jnp.bfloat16)
        partial_value = jnp.einsum("csf,sfd->csd",
                             hidden.reshape(capacity, slices, ff_dev).astype(jnp.float32),
                             down_rows.reshape(slices, ff_dev, D).astype(jnp.float32),
                             precision=lax.Precision.HIGHEST)
        rounded = lax.optimization_barrier(partial_value.astype(jnp.bfloat16))
        expert_out = jnp.sum(rounded.astype(jnp.float32), axis=1)
        expert_out = jnp.where(is_valid[:, None], expert_out, jnp.float32(0.0))
        return running.at[found_idx].add(expert_out)

    running = lax.fori_loop(0, EXPERTS, per_expert, jnp.zeros((TOKENS * 6, D), jnp.float32))
    per_pick = running.reshape(TOKENS, 3, 2, D)
    weights = gate_weight.astype(jnp.float32).reshape(TOKENS, 3, 2, 1)
    node_part = jnp.sum(weights * per_pick, axis=2).astype(jnp.bfloat16)
    return jnp.sum(node_part.astype(jnp.float32), axis=1).astype(jnp.bfloat16)
```

```python
import jax
import jax.numpy as jnp
from jax import lax
from jax.experimental import pallas as pl
from jax.experimental.pallas import tpu as pltpu
from jax.sharding import Mesh
from jax.sharding import PartitionSpec as P

EXP_NODE = 4
ALL = ("node", "e", "s")
BY_PERMUTE = True


def swap(a, axis):
    return lax.all_to_all(a, axis, split_axis=0, concat_axis=0, tiled=True)


def reorder_kernel(order, gate, up, down, gate_up, down_out):
    rows = gate.shape[0]
    gate_up[0, :rows] = gate[...]
    gate_up[0, rows:] = up[...]
    down_out[0] = down[...]


def cut_weights(order, w_gate, w_up, w_down, parts):
    rows, feature_dim = w_gate.shape
    width = feature_dim // parts
    block = pl.BlockSpec((rows, width), lambda k, order: (0, order[k]))
    return pl.pallas_call(
        reorder_kernel,
        grid_spec=pltpu.PrefetchScalarGridSpec(
            num_scalar_prefetch=1,
            grid=(parts,),
            in_specs=[block, block, block],
            out_specs=[
                pl.BlockSpec((1, 2 * rows, width), lambda k, order: (k, 0, 0)),
                pl.BlockSpec((1, rows, width), lambda k, order: (k, 0, 0)),
            ],
        ),
        out_shape=[
            jax.ShapeDtypeStruct((parts, 2 * rows, width), w_gate.dtype),
            jax.ShapeDtypeStruct((parts, rows, width), w_gate.dtype),
        ],
        name="cut_weights",
    )(order, w_gate, w_up, w_down)


def exchange(blocks, name):
    parts = blocks.shape[0]
    with jax.named_scope(name):
        if not BY_PERMUTE:
            return swap(blocks, "s")
        got = [blocks[0]]
        for k in range(1, parts):
            got.append(lax.ppermute(blocks[k], "s", [(a, a ^ k) for a in range(parts)]))
        return jnp.stack(got)


def gather(block, parts, name):
    with jax.named_scope(name):
        if not BY_PERMUTE:
            return lax.all_gather(block, "s", axis=0)
        got = [block]
        for k in range(1, parts):
            got.append(lax.ppermute(block, "s", [(a, a ^ k) for a in range(parts)]))
        return jnp.stack(got)


def on_device(tokens, node_pick, expert_pick, gate_weight, w_gate, w_up, w_down):
    node_count = lax.axis_size("node")
    slices = lax.axis_size("s")
    dev_count = EXP_NODE * slices
    tok_rows, feature_dim = tokens.shape
    width = feature_dim // slices
    slot_count = 3 * tok_rows
    cycle_len = min(node_count, max(3, slot_count // 2))
    node_cap = (slot_count + cycle_len - 1) // cycle_len
    node_slots = node_count * node_cap
    hidden_rows = w_gate.shape[0]
    all_rows = dev_count * slot_count

    order = jnp.arange(slices, dtype=jnp.int32)
    if BY_PERMUTE:
        order = order ^ lax.axis_index("s").astype(jnp.int32)
    gate_up, down = cut_weights(order, w_gate, w_up, w_down, slices)
    gate_up = exchange(gate_up, "gate_up_move")
    down = exchange(down, "down_move")

    dest_node = node_pick.reshape(slot_count)
    slot_order = jnp.arange(slot_count, dtype=jnp.int32)
    earlier = (dest_node[:, None] == dest_node[None, :]) & (
        slot_order[None, :] < slot_order[:, None]
    )
    slot_rank = jnp.sum(earlier.astype(jnp.int32), axis=1)
    position = dest_node * node_cap + slot_rank
    place = jnp.arange(node_slots, dtype=jnp.int32)[:, None] == position[None, :]
    local_pick = expert_pick.reshape(tok_rows, 3, 2)
    weights = gate_weight.reshape(tok_rows, 3, 2).astype(jnp.float32)
    chosen = (local_pick[..., None] == jnp.arange(EXP_NODE, dtype=jnp.int32)).astype(jnp.float32)
    slot_meta = (
        jnp.sum(weights[..., None] * chosen, axis=2)
        .reshape(slot_count, EXP_NODE)
        .astype(jnp.bfloat16)
    )
    slot_rows = jnp.concatenate([jnp.repeat(tokens, 3, axis=0), slot_meta], axis=1)
    sent = jnp.dot(place.astype(jnp.bfloat16), slot_rows, preferred_element_type=jnp.float32)
    sent = sent.astype(jnp.bfloat16).reshape(node_count, node_cap, feature_dim + EXP_NODE)
    with jax.named_scope("node_out_move"):
        got = swap(sent, "node").reshape(node_slots, feature_dim + EXP_NODE)
    got_meta = got[:, feature_dim:]
    is_live = got_meta > 0
    live_rank = jnp.cumsum(is_live.astype(jnp.int32), axis=0) - 1
    cap_ids = jnp.arange(slot_count, dtype=jnp.int32)[None, :, None]
    pick_table = is_live.T[:, None, :] & (live_rank.T[:, None, :] == cap_ids)
    pick_table = pick_table.reshape(EXP_NODE * slot_count, node_slots)
    packed = jnp.dot(
        pick_table.astype(jnp.bfloat16), got[:, :feature_dim], preferred_element_type=jnp.float32
    ).astype(jnp.bfloat16)
    quads = slot_count // 4
    outgoing = packed.reshape(EXP_NODE, quads, 4, slices, width).transpose(0, 3, 1, 2, 4)
    with jax.named_scope("dev_out_move"):
        arrived = swap(outgoing.reshape(dev_count, quads, 4, width), ("e", "s"))
    rows = arrived.reshape(all_rows, width)

    dims = (((1,), (1,)), ((), ()))
    acts = lax.dot_general(
        gate_up.reshape(slices * 2 * hidden_rows, width),
        rows,
        dims,
        preferred_element_type=jnp.float32,
    ).astype(jnp.bfloat16)
    acts = exchange(acts.reshape(slices, 2 * hidden_rows, all_rows), "act_move")
    acts = jnp.sum(acts.astype(jnp.float32), axis=0)
    hidden = (jax.nn.silu(acts[:hidden_rows]) * acts[hidden_rows:]).astype(jnp.bfloat16)
    hidden = gather(hidden, slices, "hidden_move").reshape(slices * hidden_rows, all_rows)
    made = lax.dot_general(
        hidden,
        down.reshape(slices * hidden_rows, width),
        (((0,), (0,)), ((), ())),
        preferred_element_type=jnp.float32,
    ).astype(jnp.bfloat16)
    with jax.named_scope("dev_back_move"):
        returned = swap(made.reshape(dev_count, quads, 4, width), ("e", "s"))
    expert_out = returned.reshape(EXP_NODE, slices, slot_count, width).transpose(0, 2, 1, 3)
    expert_out = expert_out.reshape(EXP_NODE * slot_count, feature_dim)
    combine = pick_table.T.astype(jnp.bfloat16) * jnp.repeat(got_meta, slot_count, axis=1)
    node_out = jnp.dot(combine, expert_out, preferred_element_type=jnp.float32)
    node_out = node_out.astype(jnp.bfloat16).reshape(node_count, node_cap, feature_dim)
    with jax.named_scope("node_back_move"):
        home_rows = swap(node_out, "node").reshape(node_slots, feature_dim)
    home = jnp.sum(place.reshape(node_slots, tok_rows, 3).astype(jnp.bfloat16), axis=2)
    return jnp.dot(home.T, home_rows, preferred_element_type=jnp.float32).astype(jnp.bfloat16)


def solution(mesh):
    slices = mesh.shape["dev"] // EXP_NODE
    fine = Mesh(mesh.devices.reshape(mesh.shape["node"], EXP_NODE, slices), ALL)
    spec = P(ALL, None)
    return jax.shard_map(
        on_device, mesh=fine, in_specs=(spec,) * 7, out_specs=spec, check_vma=False
    )
```

```python
import jax
import jax.numpy as jnp
from jax import lax
from jax.experimental import pallas as pl
from jax.experimental.pallas import tpu as pltpu
from jax.sharding import Mesh
from jax.sharding import PartitionSpec as P


EXP_NODE = 4
ALL = ("node", "e", "s")


def swap(a, axis):
    return lax.all_to_all(a, axis, split_axis=0, concat_axis=0, tiled=True)


def cut_kernel(order, gate, up, down, *refs):
    outs, sem = refs[:-1], refs[-1]
    parts = len(outs)
    rows = gate.shape[0]
    width = gate.shape[1] // parts
    copies = []
    for k in range(parts):
        column = pl.multiple_of(order[k] * width, width)
        for i, source in enumerate((gate, up, down)):
            copies.append(
                pltpu.make_async_copy(
                    source.at[:, pl.ds(column, width)],
                    outs[k].at[pl.ds(i * rows, rows), :],
                    sem.at[3 * k + i],
                )
            )
    for copy in copies:
        copy.start()
    for copy in copies:
        copy.wait()


def cut_weights(order, w_gate, w_up, w_down, parts):
    rows, feature_dim = w_gate.shape
    width = feature_dim // parts
    anywhere = pl.BlockSpec(memory_space=pl.ANY)
    return pl.pallas_call(
        cut_kernel,
        in_specs=[pl.BlockSpec(memory_space=pltpu.SMEM)] + [anywhere] * 3,
        out_specs=[anywhere] * parts,
        out_shape=[jax.ShapeDtypeStruct((3 * rows, width), w_gate.dtype)] * parts,
        scratch_shapes=[pltpu.SemaphoreType.DMA((3 * parts,))],
        name="cut_weights",
    )(order, w_gate, w_up, w_down)


def act_kernel(order, rows, *refs):
    blocks, out = refs[:-1], refs[-1]
    weights = jnp.concatenate([block[...] for block in blocks], axis=0)
    made = lax.dot_general(
        weights, rows[...], (((1,), (1,)), ((), ())), preferred_element_type=jnp.float32
    ).astype(jnp.bfloat16)
    size = blocks[0].shape[0]
    for k in range(len(blocks)):
        out[order[k]] = made[k * size : (k + 1) * size]


def partial_acts(order, rows, blocks):
    all_rows, width = rows.shape
    size = blocks[0].shape[0] // 3 * 2
    parts = len(blocks)
    return pl.pallas_call(
        act_kernel,
        grid=(1,),
        in_specs=[
            pl.BlockSpec(memory_space=pltpu.SMEM),
            pl.BlockSpec((all_rows, width), lambda i: (0, 0)),
        ]
        + [pl.BlockSpec((size, width), lambda i: (0, 0))] * parts,
        out_specs=pl.BlockSpec((parts, size, all_rows), lambda i: (0, 0, 0)),
        out_shape=jax.ShapeDtypeStruct((parts, size, all_rows), jnp.bfloat16),
        name="partial_acts",
    )(order, rows, *blocks)


def down_kernel(order, hidden, *refs):
    blocks, out = refs[:-1], refs[-1]
    weights = jnp.concatenate([block[...] for block in blocks], axis=0)
    units = jnp.concatenate([hidden[order[k]] for k in range(len(blocks))], axis=0)
    out[...] = lax.dot_general(
        units, weights, (((0,), (0,)), ((), ())), preferred_element_type=jnp.float32
    ).astype(jnp.bfloat16)


def down_rows(order, hidden, blocks):
    parts, size, all_rows = hidden.shape
    width = blocks[0].shape[1]
    return pl.pallas_call(
        down_kernel,
        grid=(1,),
        in_specs=[
            pl.BlockSpec(memory_space=pltpu.SMEM),
            pl.BlockSpec((parts, size, all_rows), lambda i: (0, 0, 0)),
        ]
        + [pl.BlockSpec((size, width), lambda i: (2, 0))] * parts,
        out_specs=pl.BlockSpec((all_rows, width), lambda i: (0, 0)),
        out_shape=jax.ShapeDtypeStruct((all_rows, width), jnp.bfloat16),
        name="down_rows",
    )(order, hidden, *blocks)


def on_device(tokens, node_pick, expert_pick, gate_weight, w_gate, w_up, w_down):
    node_count = lax.axis_size("node")
    slices = lax.axis_size("s")
    dev_count = EXP_NODE * slices
    tok_rows, feature_dim = tokens.shape
    width = feature_dim // slices
    slot_count = 3 * tok_rows
    cycle_len = min(node_count, max(3, slot_count // 2))
    node_cap = (slot_count + cycle_len - 1) // cycle_len
    node_slots = node_count * node_cap
    hidden_rows = w_gate.shape[0]
    all_rows = dev_count * slot_count

    order = jnp.arange(slices, dtype=jnp.int32) ^ lax.axis_index("s").astype(jnp.int32)
    cut = cut_weights(order, w_gate, w_up, w_down, slices)
    blocks = [cut[0]]
    for k in range(1, slices):
        blocks.append(lax.ppermute(cut[k], "s", [(a, a ^ k) for a in range(slices)]))

    dest_node = node_pick.reshape(slot_count)
    slot_order = jnp.arange(slot_count, dtype=jnp.int32)
    earlier = (dest_node[:, None] == dest_node[None, :]) & (
        slot_order[None, :] < slot_order[:, None]
    )
    slot_rank = jnp.sum(earlier.astype(jnp.int32), axis=1)
    position = dest_node * node_cap + slot_rank
    place = jnp.arange(node_slots, dtype=jnp.int32)[:, None] == position[None, :]
    home = jnp.sum(place.reshape(node_slots, tok_rows, 3).astype(jnp.bfloat16), axis=2)
    local_pick = expert_pick.reshape(tok_rows, 3, 2)
    weights = gate_weight.reshape(tok_rows, 3, 2).astype(jnp.float32)
    chosen = (local_pick[..., None] == jnp.arange(EXP_NODE, dtype=jnp.int32)).astype(jnp.float32)
    slot_meta = (
        jnp.sum(weights[..., None] * chosen, axis=2)
        .reshape(slot_count, EXP_NODE)
        .astype(jnp.bfloat16)
    )
    slot_rows = jnp.concatenate([jnp.repeat(tokens, 3, axis=0), slot_meta], axis=1)
    sent = jnp.dot(place.astype(jnp.bfloat16), slot_rows, preferred_element_type=jnp.float32)
    sent = sent.astype(jnp.bfloat16).reshape(node_count, node_cap, feature_dim + EXP_NODE)
    got = swap(sent, "node").reshape(node_slots, feature_dim + EXP_NODE)
    got_meta = got[:, feature_dim:]
    is_live = got_meta > 0
    live_rank = jnp.cumsum(is_live.astype(jnp.int32), axis=0) - 1
    cap_ids = jnp.arange(slot_count, dtype=jnp.int32)[None, :, None]
    pick_table = is_live.T[:, None, :] & (live_rank.T[:, None, :] == cap_ids)
    pick_table = pick_table.reshape(EXP_NODE * slot_count, node_slots)
    packed = jnp.dot(
        pick_table.astype(jnp.bfloat16), got[:, :feature_dim], preferred_element_type=jnp.float32
    ).astype(jnp.bfloat16)
    quads = slot_count // 4
    outgoing = packed.reshape(EXP_NODE, quads, 4, slices, width).transpose(0, 3, 1, 2, 4)
    arrived = swap(outgoing.reshape(dev_count, quads, 4, width), ("e", "s"))
    rows = arrived.reshape(all_rows, width)

    acts = partial_acts(order, rows, blocks)
    acts = swap(acts, "s")
    acts = jnp.sum(acts.astype(jnp.float32), axis=0)
    hidden = (jax.nn.silu(acts[:hidden_rows]) * acts[hidden_rows:]).astype(jnp.bfloat16)
    hidden = lax.all_gather(hidden, "s", axis=0)
    made = down_rows(order, hidden, blocks)
    returned = swap(made.reshape(dev_count, quads, 4, width), ("e", "s"))
    expert_out = returned.reshape(EXP_NODE, slices, slot_count, width).transpose(0, 2, 1, 3)
    expert_out = expert_out.reshape(EXP_NODE * slot_count, feature_dim)
    combine = pick_table.T.astype(jnp.bfloat16) * jnp.repeat(got_meta, slot_count, axis=1)
    node_out = jnp.dot(combine, expert_out, preferred_element_type=jnp.float32)
    node_out = node_out.astype(jnp.bfloat16).reshape(node_count, node_cap, feature_dim)
    home_rows = swap(node_out, "node").reshape(node_slots, feature_dim)
    return jnp.dot(home.T, home_rows, preferred_element_type=jnp.float32).astype(jnp.bfloat16)


def solution(mesh):
    slices = mesh.shape["dev"] // EXP_NODE
    fine = Mesh(mesh.devices.reshape(mesh.shape["node"], EXP_NODE, slices), ALL)
    spec = P(ALL, None)
    return jax.shard_map(on_device, mesh=fine, in_specs=(spec,) * 7, out_specs=spec, check_vma=False)
```

```python
import jax
import jax.numpy as jnp
from jax import lax
from jax.experimental import pallas as pl
from jax.experimental.pallas import tpu as pltpu
from jax.sharding import Mesh
from jax.sharding import PartitionSpec as P


EXP_NODE = 4
ALL = ("node", "e", "s")


def swap(a, axis):
    return lax.all_to_all(a, axis, split_axis=0, concat_axis=0, tiled=True)


def cut_kernel(order, gate, up, down, *refs):
    outs, (hold, read_sem, write_sem) = refs[:-3], refs[-3:]
    parts = len(outs)
    rows = gate.shape[0]
    width = gate.shape[1] // parts
    reads = []
    for k in range(parts):
        column = pl.multiple_of(order[k] * width, width)
        for i, source in enumerate((gate, up, down)):
            reads.append(
                pltpu.make_async_copy(
                    source.at[:, pl.ds(column, width)],
                    hold.at[k, pl.ds(i * rows, rows), :],
                    read_sem.at[3 * k + i],
                )
            )
    for read in reads:
        read.start()
    writes = []
    for k in range(parts):
        for read in reads[3 * k : 3 * k + 3]:
            read.wait()
        writes.append(pltpu.make_async_copy(hold.at[k], outs[k], write_sem.at[k]))
        writes[-1].start()
    for write in writes:
        write.wait()


def cut_weights(order, w_gate, w_up, w_down, parts):
    rows, feature_dim = w_gate.shape
    width = feature_dim // parts
    anywhere = pl.BlockSpec(memory_space=pl.ANY)
    return pl.pallas_call(
        cut_kernel,
        in_specs=[pl.BlockSpec(memory_space=pltpu.SMEM)] + [anywhere] * 3,
        out_specs=[anywhere] * parts,
        out_shape=[jax.ShapeDtypeStruct((3 * rows, width), w_gate.dtype)] * parts,
        scratch_shapes=[
            pltpu.VMEM((parts, 3 * rows, width), w_gate.dtype),
            pltpu.SemaphoreType.DMA((3 * parts,)),
            pltpu.SemaphoreType.DMA((parts,)),
        ],
        name="cut_weights",
    )(order, w_gate, w_up, w_down)


def act_kernel(order, rows, *refs):
    blocks, out = refs[:-1], refs[-1]
    weights = jnp.concatenate([block[...] for block in blocks], axis=0)
    made = lax.dot_general(
        weights, rows[...], (((1,), (1,)), ((), ())), preferred_element_type=jnp.float32
    ).astype(jnp.bfloat16)
    size = blocks[0].shape[0]
    for k in range(len(blocks)):
        out[order[k]] = made[k * size : (k + 1) * size]


def partial_acts(order, rows, blocks):
    all_rows, width = rows.shape
    size = blocks[0].shape[0] // 3 * 2
    parts = len(blocks)
    return pl.pallas_call(
        act_kernel,
        grid=(1,),
        in_specs=[
            pl.BlockSpec(memory_space=pltpu.SMEM),
            pl.BlockSpec((all_rows, width), lambda i: (0, 0)),
        ]
        + [pl.BlockSpec((size, width), lambda i: (0, 0))] * parts,
        out_specs=pl.BlockSpec((parts, size, all_rows), lambda i: (0, 0, 0)),
        out_shape=jax.ShapeDtypeStruct((parts, size, all_rows), jnp.bfloat16),
        name="partial_acts",
    )(order, rows, *blocks)


def down_kernel(order, hidden, *refs):
    blocks, out = refs[:-1], refs[-1]
    weights = jnp.concatenate([block[...] for block in blocks], axis=0)
    units = jnp.concatenate([hidden[order[k]] for k in range(len(blocks))], axis=0)
    out[...] = lax.dot_general(
        units, weights, (((0,), (0,)), ((), ())), preferred_element_type=jnp.float32
    ).astype(jnp.bfloat16)


def down_rows(order, hidden, blocks):
    parts, size, all_rows = hidden.shape
    width = blocks[0].shape[1]
    return pl.pallas_call(
        down_kernel,
        grid=(1,),
        in_specs=[
            pl.BlockSpec(memory_space=pltpu.SMEM),
            pl.BlockSpec((parts, size, all_rows), lambda i: (0, 0, 0)),
        ]
        + [pl.BlockSpec((size, width), lambda i: (2, 0))] * parts,
        out_specs=pl.BlockSpec((all_rows, width), lambda i: (0, 0)),
        out_shape=jax.ShapeDtypeStruct((all_rows, width), jnp.bfloat16),
        name="down_rows",
    )(order, hidden, *blocks)


def on_device(tokens, node_pick, expert_pick, gate_weight, w_gate, w_up, w_down):
    node_count = lax.axis_size("node")
    slices = lax.axis_size("s")
    dev_count = EXP_NODE * slices
    tok_rows, feature_dim = tokens.shape
    width = feature_dim // slices
    slot_count = 3 * tok_rows
    cycle_len = min(node_count, max(3, slot_count // 2))
    node_cap = (slot_count + cycle_len - 1) // cycle_len
    node_slots = node_count * node_cap
    hidden_rows = w_gate.shape[0]
    all_rows = dev_count * slot_count

    order = jnp.arange(slices, dtype=jnp.int32) ^ lax.axis_index("s").astype(jnp.int32)
    cut = cut_weights(order, w_gate, w_up, w_down, slices)
    blocks = [cut[0]]
    for k in range(1, slices):
        blocks.append(lax.ppermute(cut[k], "s", [(a, a ^ k) for a in range(slices)]))

    dest_node = node_pick.reshape(slot_count)
    slot_order = jnp.arange(slot_count, dtype=jnp.int32)
    earlier = (dest_node[:, None] == dest_node[None, :]) & (
        slot_order[None, :] < slot_order[:, None]
    )
    slot_rank = jnp.sum(earlier.astype(jnp.int32), axis=1)
    position = dest_node * node_cap + slot_rank
    place = jnp.arange(node_slots, dtype=jnp.int32)[:, None] == position[None, :]
    home = jnp.sum(place.reshape(node_slots, tok_rows, 3).astype(jnp.bfloat16), axis=2)
    local_pick = expert_pick.reshape(tok_rows, 3, 2)
    weights = gate_weight.reshape(tok_rows, 3, 2).astype(jnp.float32)
    chosen = (local_pick[..., None] == jnp.arange(EXP_NODE, dtype=jnp.int32)).astype(jnp.float32)
    slot_meta = (
        jnp.sum(weights[..., None] * chosen, axis=2)
        .reshape(slot_count, EXP_NODE)
        .astype(jnp.bfloat16)
    )
    slot_rows = jnp.concatenate([jnp.repeat(tokens, 3, axis=0), slot_meta], axis=1)
    sent = jnp.dot(place.astype(jnp.bfloat16), slot_rows, preferred_element_type=jnp.float32)
    sent = sent.astype(jnp.bfloat16).reshape(node_count, node_cap, feature_dim + EXP_NODE)
    got = swap(sent, "node").reshape(node_slots, feature_dim + EXP_NODE)
    got_meta = got[:, feature_dim:]
    is_live = got_meta > 0
    live_rank = jnp.cumsum(is_live.astype(jnp.int32), axis=0) - 1
    cap_ids = jnp.arange(slot_count, dtype=jnp.int32)[None, :, None]
    pick_table = is_live.T[:, None, :] & (live_rank.T[:, None, :] == cap_ids)
    pick_table = pick_table.reshape(EXP_NODE * slot_count, node_slots)
    packed = jnp.dot(
        pick_table.astype(jnp.bfloat16), got[:, :feature_dim], preferred_element_type=jnp.float32
    ).astype(jnp.bfloat16)
    quads = slot_count // 4
    outgoing = packed.reshape(EXP_NODE, quads, 4, slices, width).transpose(0, 3, 1, 2, 4)
    arrived = swap(outgoing.reshape(dev_count, quads, 4, width), ("e", "s"))
    rows = arrived.reshape(all_rows, width)

    acts = partial_acts(order, rows, blocks)
    acts = swap(acts, "s")
    acts = jnp.sum(acts.astype(jnp.float32), axis=0)
    hidden = (jax.nn.silu(acts[:hidden_rows]) * acts[hidden_rows:]).astype(jnp.bfloat16)
    hidden = lax.all_gather(hidden, "s", axis=0)
    made = down_rows(order, hidden, blocks)
    returned = swap(made.reshape(dev_count, quads, 4, width), ("e", "s"))
    expert_out = returned.reshape(EXP_NODE, slices, slot_count, width).transpose(0, 2, 1, 3)
    expert_out = expert_out.reshape(EXP_NODE * slot_count, feature_dim)
    combine = pick_table.T.astype(jnp.bfloat16) * jnp.repeat(got_meta, slot_count, axis=1)
    node_out = jnp.dot(combine, expert_out, preferred_element_type=jnp.float32)
    node_out = node_out.astype(jnp.bfloat16).reshape(node_count, node_cap, feature_dim)
    home_rows = swap(node_out, "node").reshape(node_slots, feature_dim)
    return jnp.dot(home.T, home_rows, preferred_element_type=jnp.float32).astype(jnp.bfloat16)


def solution(mesh):
    slices = mesh.shape["dev"] // EXP_NODE
    fine = Mesh(mesh.devices.reshape(mesh.shape["node"], EXP_NODE, slices), ALL)
    spec = P(ALL, None)
    return jax.shard_map(on_device, mesh=fine, in_specs=(spec,) * 7, out_specs=spec, check_vma=False)
```

```python
import jax
import jax.numpy as jnp
from jax import lax
from jax.experimental import pallas as pl
from jax.experimental.pallas import tpu as pltpu
from jax.sharding import Mesh
from jax.sharding import PartitionSpec as P


EXP_NODE = 4
ALL = ("node", "e", "s")
FIRST = (6, 4, 2, 7)
THEN = (5, 3, 1)


def swap(a, axis):
    return lax.all_to_all(a, axis, split_axis=0, concat_axis=0, tiled=True)


def cut_kernel(order, gate, up, down, *refs):
    outs, (hold, read_sem, write_sem) = refs[:-3], refs[-3:]
    parts = len(outs)
    rows = gate.shape[0]
    width = gate.shape[1] // parts
    reads = []
    for k in range(parts):
        column = pl.multiple_of(order[k] * width, width)
        for i, source in enumerate((gate, up, down)):
            reads.append(
                pltpu.make_async_copy(
                    source.at[:, pl.ds(column, width)],
                    hold.at[k, pl.ds(i * rows, rows), :],
                    read_sem.at[3 * k + i],
                )
            )
    for read in reads:
        read.start()
    writes = []
    for k in range(parts):
        for read in reads[3 * k : 3 * k + 3]:
            read.wait()
        writes.append(pltpu.make_async_copy(hold.at[k], outs[k], write_sem.at[k]))
        writes[-1].start()
    for write in writes:
        write.wait()


def cut_weights(order, w_gate, w_up, w_down, parts):
    rows, feature_dim = w_gate.shape
    width = feature_dim // parts
    anywhere = pl.BlockSpec(memory_space=pl.ANY)
    return pl.pallas_call(
        cut_kernel,
        in_specs=[pl.BlockSpec(memory_space=pltpu.SMEM)] + [anywhere] * 3,
        out_specs=[anywhere] * parts,
        out_shape=[jax.ShapeDtypeStruct((3 * rows, width), w_gate.dtype)] * parts,
        scratch_shapes=[
            pltpu.VMEM((parts, 3 * rows, width), w_gate.dtype),
            pltpu.SemaphoreType.DMA((3 * parts,)),
            pltpu.SemaphoreType.DMA((parts,)),
        ],
        name="cut_weights",
    )(order, w_gate, w_up, w_down)


def act_kernel(order, rows, *refs):
    blocks, (out, hold, sem) = refs[:-3], refs[-3:]
    parts, size = out.shape[:2]
    reads = []
    for k in range(parts):
        target = hold.at[pl.ds(k * size, size), :]
        reads.append(pltpu.make_async_copy(blocks[k].at[pl.ds(0, size), :], target, sem.at[k]))
    for read in reads:
        read.start()
    half = parts // 2
    for low in range(0, parts, half):
        for read in reads[low : low + half]:
            read.wait()
        made = lax.dot_general(
            hold[low * size : (low + half) * size],
            rows[...],
            (((1,), (1,)), ((), ())),
            preferred_element_type=jnp.float32,
        ).astype(jnp.bfloat16)
        for k in range(half):
            out[order[low + k]] = made[k * size : (k + 1) * size]


def partial_acts(order, rows, blocks):
    all_rows, width = rows.shape
    size = blocks[0].shape[0] // 3 * 2
    parts = len(blocks)
    return pl.pallas_call(
        act_kernel,
        in_specs=[
            pl.BlockSpec(memory_space=pltpu.SMEM),
            pl.BlockSpec(memory_space=pltpu.VMEM),
        ]
        + [pl.BlockSpec(memory_space=pl.ANY)] * parts,
        out_specs=pl.BlockSpec(memory_space=pltpu.VMEM),
        out_shape=jax.ShapeDtypeStruct((parts, size, all_rows), jnp.bfloat16),
        scratch_shapes=[
            pltpu.VMEM((parts * size, width), jnp.bfloat16),
            pltpu.SemaphoreType.DMA((parts,)),
        ],
        name="partial_acts",
    )(order, rows, *blocks)


def down_kernel(order, hidden, *refs):
    blocks, out = refs[:-1], refs[-1]
    weights = jnp.concatenate([block[...] for block in blocks], axis=0)
    units = jnp.concatenate([hidden[order[k]] for k in range(len(blocks))], axis=0)
    out[...] = lax.dot_general(
        units, weights, (((0,), (0,)), ((), ())), preferred_element_type=jnp.float32
    ).astype(jnp.bfloat16)


def down_rows(order, hidden, blocks):
    parts, size, all_rows = hidden.shape
    width = blocks[0].shape[1]
    return pl.pallas_call(
        down_kernel,
        grid=(1,),
        in_specs=[
            pl.BlockSpec(memory_space=pltpu.SMEM),
            pl.BlockSpec((parts, size, all_rows), lambda i: (0, 0, 0)),
        ]
        + [pl.BlockSpec((size, width), lambda i: (2, 0))] * parts,
        out_specs=pl.BlockSpec((all_rows, width), lambda i: (0, 0)),
        out_shape=jax.ShapeDtypeStruct((all_rows, width), jnp.bfloat16),
        name="down_rows",
    )(order, hidden, *blocks)


def on_device(tokens, node_pick, expert_pick, gate_weight, w_gate, w_up, w_down):
    node_count = lax.axis_size("node")
    slices = lax.axis_size("s")
    dev_count = EXP_NODE * slices
    tok_rows, feature_dim = tokens.shape
    width = feature_dim // slices
    slot_count = 3 * tok_rows
    cycle_len = min(node_count, max(3, slot_count // 2))
    node_cap = (slot_count + cycle_len - 1) // cycle_len
    node_slots = node_count * node_cap
    hidden_rows = w_gate.shape[0]
    all_rows = dev_count * slot_count

    order = jnp.arange(slices, dtype=jnp.int32) ^ lax.axis_index("s").astype(jnp.int32)
    cut = cut_weights(order, w_gate, w_up, w_down, slices)
    blocks = list(cut)
    for steps in (FIRST, THEN):
        for k in steps:
            blocks[k] = lax.ppermute(cut[k], "s", [(a, a ^ k) for a in range(slices)])

    dest_node = node_pick.reshape(slot_count)
    slot_order = jnp.arange(slot_count, dtype=jnp.int32)
    earlier = (dest_node[:, None] == dest_node[None, :]) & (
        slot_order[None, :] < slot_order[:, None]
    )
    slot_rank = jnp.sum(earlier.astype(jnp.int32), axis=1)
    position = dest_node * node_cap + slot_rank
    place = jnp.arange(node_slots, dtype=jnp.int32)[:, None] == position[None, :]
    by_token = place.reshape(node_slots, tok_rows, 3).astype(jnp.bfloat16)
    home = lax.optimization_barrier(by_token[..., 0] + by_token[..., 1])
    home = lax.optimization_barrier(home + by_token[..., 2])
    local_pick = expert_pick.reshape(tok_rows, 3, 2)
    weights = gate_weight.reshape(tok_rows, 3, 2).astype(jnp.float32)
    chosen = (local_pick[..., None] == jnp.arange(EXP_NODE, dtype=jnp.int32)).astype(jnp.float32)
    slot_meta = (
        jnp.sum(weights[..., None] * chosen, axis=2)
        .reshape(slot_count, EXP_NODE)
        .astype(jnp.bfloat16)
    )
    slot_rows = jnp.concatenate([jnp.repeat(tokens, 3, axis=0), slot_meta], axis=1)
    sent = jnp.dot(place.astype(jnp.bfloat16), slot_rows, preferred_element_type=jnp.float32)
    sent = sent.astype(jnp.bfloat16).reshape(node_count, node_cap, feature_dim + EXP_NODE)
    got = swap(sent, "node").reshape(node_slots, feature_dim + EXP_NODE)
    got_meta = got[:, feature_dim:]
    is_live = got_meta > 0
    live_rank = jnp.cumsum(is_live.astype(jnp.int32), axis=0) - 1
    cap_ids = jnp.arange(slot_count, dtype=jnp.int32)[None, :, None]
    pick_table = is_live.T[:, None, :] & (live_rank.T[:, None, :] == cap_ids)
    pick_table = pick_table.reshape(EXP_NODE * slot_count, node_slots)
    packed = jnp.dot(
        pick_table.astype(jnp.bfloat16), got[:, :feature_dim], preferred_element_type=jnp.float32
    ).astype(jnp.bfloat16)
    quads = slot_count // 4
    outgoing = packed.reshape(EXP_NODE, quads, 4, slices, width).transpose(0, 3, 1, 2, 4)
    arrived = swap(outgoing.reshape(dev_count, quads, 4, width), ("e", "s"))
    rows = arrived.reshape(all_rows, width)

    acts = partial_acts(order, rows, blocks)
    acts = swap(acts, "s")
    acts = jnp.sum(acts.astype(jnp.float32), axis=0)
    hidden = (jax.nn.silu(acts[:hidden_rows]) * acts[hidden_rows:]).astype(jnp.bfloat16)
    hidden = lax.all_gather(hidden, "s", axis=0)
    made = down_rows(order, hidden, blocks)
    returned = swap(made.reshape(dev_count, quads, 4, width), ("e", "s"))
    expert_out = returned.reshape(EXP_NODE, slices, slot_count, width).transpose(0, 2, 1, 3)
    expert_out = expert_out.reshape(EXP_NODE * slot_count, feature_dim)
    combine = pick_table.T.astype(jnp.bfloat16) * jnp.repeat(got_meta, slot_count, axis=1)
    node_out = jnp.dot(combine, expert_out, preferred_element_type=jnp.float32)
    node_out = node_out.astype(jnp.bfloat16).reshape(node_count, node_cap, feature_dim)
    home_rows = swap(node_out, "node").reshape(node_slots, feature_dim)
    return jnp.dot(home.T, home_rows, preferred_element_type=jnp.float32).astype(jnp.bfloat16)


def solution(mesh):
    slices = mesh.shape["dev"] // EXP_NODE
    fine = Mesh(mesh.devices.reshape(mesh.shape["node"], EXP_NODE, slices), ALL)
    spec = P(ALL, None)
    return jax.shard_map(on_device, mesh=fine, in_specs=(spec,) * 7, out_specs=spec, check_vma=False)
```

```python
import jax
import jax.numpy as jnp
from jax import lax
from jax.experimental import pallas as pl
from jax.experimental.pallas import tpu as pltpu
from jax.sharding import Mesh
from jax.sharding import PartitionSpec as P


EXP_NODE = 4
ALL = ("node", "e", "q", "c")
PART = ("q", "c")
STEPS = (0, 6, 4, 2, 7, 5, 3, 1)
FIRST = (1, 2, 3, 4)
THEN = (5, 6, 7)


def swap(a, axis):
    return lax.all_to_all(a, axis, split_axis=0, concat_axis=0, tiled=True)


def cut_kernel(order, gate, up, down, *refs):
    outs, (hold, read_sem, write_sem) = refs[:-3], refs[-3:]
    parts = len(outs)
    rows = gate.shape[0]
    width = gate.shape[1] // parts
    reads = []
    for k in range(parts):
        column = pl.multiple_of(order[k] * width, width)
        for i, source in enumerate((gate, up, down)):
            reads.append(
                pltpu.make_async_copy(
                    source.at[:, pl.ds(column, width)],
                    hold.at[k, pl.ds(i * rows, rows), :],
                    read_sem.at[3 * k + i],
                )
            )
    for read in reads:
        read.start()
    writes = []
    for k in range(parts):
        for read in reads[3 * k : 3 * k + 3]:
            read.wait()
        writes.append(pltpu.make_async_copy(hold.at[k], outs[k], write_sem.at[k]))
        writes[-1].start()
    for write in writes:
        write.wait()


def cut_weights(order, w_gate, w_up, w_down, parts):
    rows, feature_dim = w_gate.shape
    width = feature_dim // parts
    anywhere = pl.BlockSpec(memory_space=pl.ANY)
    return pl.pallas_call(
        cut_kernel,
        in_specs=[pl.BlockSpec(memory_space=pltpu.SMEM)] + [anywhere] * 3,
        out_specs=[anywhere] * parts,
        out_shape=[jax.ShapeDtypeStruct((3 * rows, width), w_gate.dtype)] * parts,
        scratch_shapes=[
            pltpu.VMEM((parts, 3 * rows, width), w_gate.dtype),
            pltpu.SemaphoreType.DMA((3 * parts,)),
            pltpu.SemaphoreType.DMA((parts,)),
        ],
        name="cut_weights",
    )(order, w_gate, w_up, w_down)


def act_kernel(order, rows, *refs):
    blocks, out = refs[:-1], refs[-1]
    weights = jnp.concatenate([block[...] for block in blocks], axis=0)
    made = lax.dot_general(
        weights, rows[...], (((1,), (1,)), ((), ())), preferred_element_type=jnp.float32
    ).astype(jnp.bfloat16)
    size = blocks[0].shape[0]
    for k in range(len(blocks)):
        out[order[k]] = made[k * size : (k + 1) * size]


def partial_acts(order, rows, blocks):
    all_rows, width = rows.shape
    size = blocks[0].shape[0] // 3 * 2
    parts = len(blocks)
    return pl.pallas_call(
        act_kernel,
        grid=(all_rows // 128,),
        in_specs=[
            pl.BlockSpec(memory_space=pltpu.SMEM),
            pl.BlockSpec((128, width), lambda i: (i, 0)),
        ]
        + [pl.BlockSpec((size, width), lambda i: (0, 0))] * parts,
        out_specs=pl.BlockSpec((parts, size, 128), lambda i: (0, 0, i)),
        out_shape=jax.ShapeDtypeStruct((parts, size, all_rows), jnp.bfloat16),
        name="partial_acts",
    )(order, rows, *blocks)


def down_kernel(order, mine, other, *refs):
    blocks, out = refs[:-1], refs[-1]
    weights = jnp.concatenate([block[...] for block in blocks], axis=0)
    held = [other if STEPS[k] % 2 else mine for k in range(len(blocks))]
    units = jnp.concatenate([held[k][order[k] // 2] for k in range(len(blocks))], axis=0)
    out[...] = lax.dot_general(
        units, weights, (((0,), (0,)), ((), ())), preferred_element_type=jnp.float32
    ).astype(jnp.bfloat16)


def down_rows(order, mine, other, blocks):
    chips, size, all_rows = mine.shape
    parts = len(blocks)
    width = blocks[0].shape[1]
    return pl.pallas_call(
        down_kernel,
        grid=(1,),
        in_specs=[
            pl.BlockSpec(memory_space=pltpu.SMEM),
            pl.BlockSpec((chips, size, all_rows), lambda i: (0, 0, 0)),
            pl.BlockSpec((chips, size, all_rows), lambda i: (0, 0, 0)),
        ]
        + [pl.BlockSpec((size, width), lambda i: (2, 0))] * parts,
        out_specs=pl.BlockSpec((all_rows, width), lambda i: (0, 0)),
        out_shape=jax.ShapeDtypeStruct((all_rows, width), jnp.bfloat16),
        name="down_rows",
    )(order, mine, other, *blocks)


def on_device(tokens, node_pick, expert_pick, gate_weight, w_gate, w_up, w_down):
    node_count = lax.axis_size("node")
    slices = lax.axis_size(PART)
    dev_count = EXP_NODE * slices
    tok_rows, feature_dim = tokens.shape
    width = feature_dim // slices
    slot_count = 3 * tok_rows
    cycle_len = min(node_count, max(3, slot_count // 2))
    node_cap = (slot_count + cycle_len - 1) // cycle_len
    node_slots = node_count * node_cap
    hidden_rows = w_gate.shape[0]
    all_rows = dev_count * slot_count

    order = jnp.array(STEPS, jnp.int32) ^ lax.axis_index(PART).astype(jnp.int32)
    cut = cut_weights(order, w_gate, w_up, w_down, slices)
    blocks = list(cut)
    for steps in (FIRST, THEN):
        for k in steps:
            pairs = [(a, a ^ STEPS[k]) for a in range(slices)]
            blocks[k] = lax.ppermute(cut[k], PART, pairs)

    dest_node = node_pick.reshape(slot_count)
    slot_order = jnp.arange(slot_count, dtype=jnp.int32)
    earlier = (dest_node[:, None] == dest_node[None, :]) & (
        slot_order[None, :] < slot_order[:, None]
    )
    slot_rank = jnp.sum(earlier.astype(jnp.int32), axis=1)
    position = dest_node * node_cap + slot_rank
    place = jnp.arange(node_slots, dtype=jnp.int32)[:, None] == position[None, :]
    by_token = place.reshape(node_slots, tok_rows, 3).astype(jnp.bfloat16)
    home = lax.optimization_barrier(by_token[..., 0] + by_token[..., 1])
    home = lax.optimization_barrier(home + by_token[..., 2])
    local_pick = expert_pick.reshape(tok_rows, 3, 2)
    weights = gate_weight.reshape(tok_rows, 3, 2).astype(jnp.float32)
    chosen = (local_pick[..., None] == jnp.arange(EXP_NODE, dtype=jnp.int32)).astype(jnp.float32)
    slot_meta = (
        jnp.sum(weights[..., None] * chosen, axis=2)
        .reshape(slot_count, EXP_NODE)
        .astype(jnp.bfloat16)
    )
    slot_rows = jnp.concatenate([jnp.repeat(tokens, 3, axis=0), slot_meta], axis=1)
    sent = jnp.dot(place.astype(jnp.bfloat16), slot_rows, preferred_element_type=jnp.float32)
    sent = sent.astype(jnp.bfloat16).reshape(node_count, node_cap, feature_dim + EXP_NODE)
    got = swap(sent, "node").reshape(node_slots, feature_dim + EXP_NODE)
    got_meta = got[:, feature_dim:]
    is_live = got_meta > 0
    live_rank = jnp.cumsum(is_live.astype(jnp.int32), axis=0) - 1
    cap_ids = jnp.arange(slot_count, dtype=jnp.int32)[None, :, None]
    pick_table = is_live.T[:, None, :] & (live_rank.T[:, None, :] == cap_ids)
    pick_table = pick_table.reshape(EXP_NODE * slot_count, node_slots)
    packed = jnp.dot(
        pick_table.astype(jnp.bfloat16), got[:, :feature_dim], preferred_element_type=jnp.float32
    ).astype(jnp.bfloat16)
    quads = slot_count // 4
    outgoing = packed.reshape(EXP_NODE, quads, 4, slices, width).transpose(0, 3, 1, 2, 4)
    arrived = swap(outgoing.reshape(dev_count, quads, 4, width), ("e", *PART))
    rows = arrived.reshape(all_rows, width)

    acts = partial_acts(order, rows, blocks)
    acts = swap(acts, PART)
    acts = jnp.sum(acts.astype(jnp.float32), axis=0)
    hidden = (jax.nn.silu(acts[:hidden_rows]) * acts[hidden_rows:]).astype(jnp.bfloat16)
    mine = lax.all_gather(hidden, "q", axis=0)
    other = lax.ppermute(mine, "c", [(0, 1), (1, 0)])
    made = down_rows(order, mine, other, blocks)
    returned = swap(made.reshape(dev_count, quads, 4, width), ("e", *PART))
    expert_out = returned.reshape(EXP_NODE, slices, slot_count, width).transpose(0, 2, 1, 3)
    expert_out = expert_out.reshape(EXP_NODE * slot_count, feature_dim)
    combine = pick_table.T.astype(jnp.bfloat16) * jnp.repeat(got_meta, slot_count, axis=1)
    node_out = jnp.dot(combine, expert_out, preferred_element_type=jnp.float32)
    node_out = node_out.astype(jnp.bfloat16).reshape(node_count, node_cap, feature_dim)
    home_rows = swap(node_out, "node").reshape(node_slots, feature_dim)
    return jnp.dot(home.T, home_rows, preferred_element_type=jnp.float32).astype(jnp.bfloat16)


def solution(mesh):
    slices = mesh.shape["dev"] // EXP_NODE
    fine = Mesh(mesh.devices.reshape(mesh.shape["node"], EXP_NODE, slices // 2, 2), ALL)
    spec = P(ALL, None)
    return jax.shard_map(on_device, mesh=fine, in_specs=(spec,) * 7, out_specs=spec, check_vma=False)
```

```python
import jax
import jax.numpy as jnp
from jax import lax
from jax.experimental import pallas as pl
from jax.experimental.pallas import tpu as pltpu
from jax.sharding import Mesh
from jax.sharding import PartitionSpec as P


EXP_NODE = 4
ALL = ("node", "e", "s")
FIRST = (4, 5, 6, 7)
THEN = (1, 2, 3)


def swap(a, axis):
    return lax.all_to_all(a, axis, split_axis=0, concat_axis=0, tiled=True)


def cut_kernel(order, gate, up, down, *refs):
    outs, (hold, read_sem, write_sem) = refs[:-3], refs[-3:]
    parts = len(outs)
    rows = gate.shape[0]
    width = gate.shape[1] // parts
    reads = []
    for k in range(parts):
        column = pl.multiple_of(order[k] * width, width)
        for i, source in enumerate((gate, up, down)):
            reads.append(
                pltpu.make_async_copy(
                    source.at[:, pl.ds(column, width)],
                    hold.at[k, pl.ds(i * rows, rows), :],
                    read_sem.at[3 * k + i],
                )
            )
    for read in reads:
        read.start()
    writes = []
    for k in range(parts):
        for read in reads[3 * k : 3 * k + 3]:
            read.wait()
        writes.append(pltpu.make_async_copy(hold.at[k], outs[k], write_sem.at[k]))
        writes[-1].start()
    for write in writes:
        write.wait()


def cut_weights(order, w_gate, w_up, w_down, parts):
    rows, feature_dim = w_gate.shape
    width = feature_dim // parts
    anywhere = pl.BlockSpec(memory_space=pl.ANY)
    return pl.pallas_call(
        cut_kernel,
        in_specs=[pl.BlockSpec(memory_space=pltpu.SMEM)] + [anywhere] * 3,
        out_specs=[anywhere] * parts,
        out_shape=[jax.ShapeDtypeStruct((3 * rows, width), w_gate.dtype)] * parts,
        scratch_shapes=[
            pltpu.VMEM((parts, 3 * rows, width), w_gate.dtype),
            pltpu.SemaphoreType.DMA((3 * parts,)),
            pltpu.SemaphoreType.DMA((parts,)),
        ],
        name="cut_weights",
    )(order, w_gate, w_up, w_down)


def act_kernel(order, rows, *refs):
    blocks, out = refs[:-1], refs[-1]
    weights = jnp.concatenate([block[...] for block in blocks], axis=0)
    made = lax.dot_general(
        weights, rows[...], (((1,), (1,)), ((), ())), preferred_element_type=jnp.float32
    ).astype(jnp.bfloat16)
    size = blocks[0].shape[0]
    for k in range(len(blocks)):
        out[order[k]] = made[k * size : (k + 1) * size]


def partial_acts(order, rows, blocks):
    all_rows, width = rows.shape
    size = blocks[0].shape[0] // 3 * 2
    parts = len(blocks)
    return pl.pallas_call(
        act_kernel,
        grid=(1,),
        in_specs=[
            pl.BlockSpec(memory_space=pltpu.SMEM),
            pl.BlockSpec((all_rows, width), lambda i: (0, 0)),
        ]
        + [pl.BlockSpec((size, width), lambda i: (0, 0))] * parts,
        out_specs=pl.BlockSpec((parts, size, all_rows), lambda i: (0, 0, 0)),
        out_shape=jax.ShapeDtypeStruct((parts, size, all_rows), jnp.bfloat16),
        name="partial_acts",
    )(order, rows, *blocks)


def order_kernel(order, *refs):
    blocks, out = refs[:-1], refs[-1]
    for k, block in enumerate(blocks):
        out[order[k]] = block[...]


def ordered_down(order, blocks):
    parts = len(blocks)
    size, width = blocks[0].shape[0] // 3, blocks[0].shape[1]
    return pl.pallas_call(
        order_kernel,
        grid=(1,),
        in_specs=[pl.BlockSpec(memory_space=pltpu.SMEM)]
        + [pl.BlockSpec((size, width), lambda i: (2, 0))] * parts,
        out_specs=pl.BlockSpec((parts, size, width), lambda i: (0, 0, 0)),
        out_shape=jax.ShapeDtypeStruct((parts, size, width), jnp.bfloat16),
        name="ordered_down",
    )(order, *blocks)


def on_device(tokens, node_pick, expert_pick, gate_weight, w_gate, w_up, w_down):
    node_count = lax.axis_size("node")
    slices = lax.axis_size("s")
    dev_count = EXP_NODE * slices
    tok_rows, feature_dim = tokens.shape
    width = feature_dim // slices
    slot_count = 3 * tok_rows
    cycle_len = min(node_count, max(3, slot_count // 2))
    node_cap = (slot_count + cycle_len - 1) // cycle_len
    node_slots = node_count * node_cap
    hidden_rows = w_gate.shape[0]
    all_rows = dev_count * slot_count

    order = jnp.arange(slices, dtype=jnp.int32) ^ lax.axis_index("s").astype(jnp.int32)
    cut = cut_weights(order, w_gate, w_up, w_down, slices)
    blocks = list(cut)
    for steps in (FIRST, THEN):
        for k in steps:
            blocks[k] = lax.ppermute(cut[k], "s", [(a, a ^ k) for a in range(slices)])

    dest_node = node_pick.reshape(slot_count)
    slot_order = jnp.arange(slot_count, dtype=jnp.int32)
    earlier = (dest_node[:, None] == dest_node[None, :]) & (
        slot_order[None, :] < slot_order[:, None]
    )
    slot_rank = jnp.sum(earlier.astype(jnp.int32), axis=1)
    position = dest_node * node_cap + slot_rank
    place = jnp.arange(node_slots, dtype=jnp.int32)[:, None] == position[None, :]
    by_token = place.reshape(node_slots, tok_rows, 3).astype(jnp.bfloat16)
    home = lax.optimization_barrier(by_token[..., 0] + by_token[..., 1])
    home = lax.optimization_barrier(home + by_token[..., 2])
    local_pick = expert_pick.reshape(tok_rows, 3, 2)
    weights = gate_weight.reshape(tok_rows, 3, 2).astype(jnp.float32)
    chosen = (local_pick[..., None] == jnp.arange(EXP_NODE, dtype=jnp.int32)).astype(jnp.float32)
    slot_meta = (
        jnp.sum(weights[..., None] * chosen, axis=2)
        .reshape(slot_count, EXP_NODE)
        .astype(jnp.bfloat16)
    )
    slot_rows = jnp.concatenate([jnp.repeat(tokens, 3, axis=0), slot_meta], axis=1)
    sent = jnp.dot(place.astype(jnp.bfloat16), slot_rows, preferred_element_type=jnp.float32)
    sent = sent.astype(jnp.bfloat16).reshape(node_count, node_cap, feature_dim + EXP_NODE)
    got = swap(sent, "node").reshape(node_slots, feature_dim + EXP_NODE)
    got_meta = got[:, feature_dim:]
    is_live = got_meta > 0
    live_rank = jnp.cumsum(is_live.astype(jnp.int32), axis=0) - 1
    cap_ids = jnp.arange(slot_count, dtype=jnp.int32)[None, :, None]
    pick_table = is_live.T[:, None, :] & (live_rank.T[:, None, :] == cap_ids)
    pick_table = pick_table.reshape(EXP_NODE * slot_count, node_slots)
    packed = jnp.dot(
        pick_table.astype(jnp.bfloat16), got[:, :feature_dim], preferred_element_type=jnp.float32
    ).astype(jnp.bfloat16)
    quads = slot_count // 4
    outgoing = packed.reshape(EXP_NODE, quads, 4, slices, width).transpose(0, 3, 1, 2, 4)
    arrived = swap(outgoing.reshape(dev_count, quads, 4, width), ("e", "s"))
    rows = arrived.reshape(all_rows, width)

    acts = partial_acts(order, rows, blocks)
    down = ordered_down(order, blocks).reshape(slices * hidden_rows, width)
    acts = swap(acts, "s")
    acts = jnp.sum(acts.astype(jnp.float32), axis=0)
    hidden = (jax.nn.silu(acts[:hidden_rows]) * acts[hidden_rows:]).astype(jnp.bfloat16)
    hidden = lax.all_gather(hidden, "s", axis=0, tiled=True)
    made = lax.dot_general(
        hidden, down, (((0,), (0,)), ((), ())), preferred_element_type=jnp.float32
    ).astype(jnp.bfloat16)
    returned = swap(made.reshape(dev_count, quads, 4, width), ("e", "s"))
    expert_out = returned.reshape(EXP_NODE, slices, slot_count, width).transpose(0, 2, 1, 3)
    expert_out = expert_out.reshape(EXP_NODE * slot_count, feature_dim)
    combine = pick_table.T.astype(jnp.bfloat16) * jnp.repeat(got_meta, slot_count, axis=1)
    node_out = jnp.dot(combine, expert_out, preferred_element_type=jnp.float32)
    node_out = node_out.astype(jnp.bfloat16).reshape(node_count, node_cap, feature_dim)
    home_rows = swap(node_out, "node").reshape(node_slots, feature_dim)
    return jnp.dot(home.T, home_rows, preferred_element_type=jnp.float32).astype(jnp.bfloat16)


def solution(mesh):
    slices = mesh.shape["dev"] // EXP_NODE
    fine = Mesh(mesh.devices.reshape(mesh.shape["node"], EXP_NODE, slices), ALL)
    spec = P(ALL, None)
    return jax.shard_map(on_device, mesh=fine, in_specs=(spec,) * 7, out_specs=spec, check_vma=False)
```
